32 devices in a mesh: groups: 2 (over y), rows: 4 (over z), sub: 4 (over x, core).
Axes of the slice: x: 2, y: 2, z: 4, core: 2. Of those that a mesh axis runs over, the one named last changes fastest.
Arguments:
- matrix: float32 [16384, 1024], P(('groups', 'rows', 'sub')), parts along dimension 0
- sign_bits: int32 [16384], P(('groups', 'rows', 'sub')), parts along dimension 0, may hold values from 0 to 1
- samples: int32 [8192], P('groups'), parts along dimension 0, may hold values from 0 to 8191
Outputs:
- cholesky_factor: float32 [2048, 1024], P('groups'), parts along dimension 0
The draws below stay inside these ranges and needn't reach their ends.
There are 2 independent parts, one for each index of `groups`. The reference program is written for one: setup_inputs(seed, part) draws one part's arguments, and reference() takes and returns one part's arrays. A program takes and returns all parts, laid end to end along the dimension named above; each array names one. Nothing has to cross between parts.
Inputs may be any that keep to these rules, and one draw needn't show every extreme that they name: `samples`: row numbers of the whole matrix, drawn independently; a row may be drawn more than once.
All inputs are finite; a program needn't handle non-finite values.
Results may differ from the reference program's by a relative error of at most 0.00011.
Values sent between devices are 32-bit elements; how exact they have to be, the bound alone decides.
A program may use at most 64 MiB of HBM per device.

```python
import math
import jax
import jax.numpy as jnp
from jax import lax

N = 1024
S = 4096
M = 8192


def draw_matrix(key, part):
    streams = jax.random.split(jax.random.fold_in(key, 17), 3)
    column_scale = jnp.exp(jax.random.uniform(streams[0], (N,), jnp.float32, 0.0, math.log(3.0)))
    row_scale = jnp.exp(jax.random.uniform(streams[1], (M,), jnp.float32, 0.0, math.log(10.0)))
    raw_values = jax.random.truncated_normal(streams[2], -6.0, 6.0, (M, N), jnp.float32)
    return raw_values * row_scale[:, None] * column_scale[None, :] * 0.25


def place_ends(result, own_key, low, largest):
    longest = result.shape.index(max(result.shape))
    spots = []
    for shift in (0, 1):
        where = [jax.random.randint(jax.random.fold_in(own_key, axis), (), 0, length) for axis, length in enumerate(result.shape)]
        where[longest] = (where[longest] + shift) % result.shape[longest]
        spots.append(tuple(where))
    return result.at[spots[0]].set(low).at[spots[1]].set(largest)


def setup_inputs(seed: int = 0, part: int = 0) -> dict:
    arg_keys = jax.random.split(jax.random.key(seed), 4)
    part_keys = jax.random.split(jax.random.fold_in(arg_keys[3], part), 4)
    matrix = draw_matrix(jax.random.fold_in(jax.random.fold_in(arg_keys[3], part), 71), part)
    sign_bits = place_ends(jax.random.randint(part_keys[1], (M,), 0, 2), jax.random.fold_in(part_keys[1], 1), 0, 1).astype(jnp.int32)
    samples = place_ends(jax.random.randint(part_keys[2], (S,), 0, M), jax.random.fold_in(part_keys[2], 1), 0, M - 1).astype(jnp.int32)
    return {"matrix": matrix, "sign_bits": sign_bits, "samples": samples}


def hadamard_rows(values):
    extent = values.shape[0]
    columns = values.shape[1]
    stride = 1
    for level in range(extent.bit_length() - 1):
        paired = values.reshape(extent // (2 * stride), 2, stride, columns)
        values = jnp.stack((paired[:, 0] + paired[:, 1], paired[:, 0] - paired[:, 1]), axis=1).reshape(extent, columns)
        stride = stride * 2
    return values

def reference(matrix, sign_bits, samples):
    sign_values = (2 * sign_bits - 1).astype(jnp.float32)
    signed = matrix * sign_values[:, None]
    mixed_rows = hadamard_rows(signed) / jnp.sqrt(jnp.float32(matrix.shape[0]))
    picked = jnp.take(mixed_rows, samples.astype(jnp.int32), axis=0)
    gram_matrix = jnp.dot(picked.T.astype(jnp.float32), picked.astype(jnp.float32), precision=lax.Precision.HIGHEST, preferred_element_type=jnp.float32) / jnp.float32(samples.shape[0])
    return jnp.linalg.cholesky(gram_matrix)
```

```python
import jax
import jax.numpy as jnp
from jax import lax
from jax.experimental import pallas as pl
from jax.experimental.pallas import tpu as pltpu
from jax.sharding import PartitionSpec as P

HIGHEST = lax.Precision.HIGHEST


T = 128
NT = (((1,), (1,)), ((), ()))
NN = (((1,), (0,)), ((), ()))

def factor_block(a_ref, u_ref):
    sub8 = lax.broadcasted_iota(jnp.int32, (8, T), 0)
    for r0 in range(0, T, 8):
        p = a_ref[r0:r0 + 8, :]
        left = p[:, :T]
        cols = [jnp.broadcast_to(left[:, r0 + j:r0 + j + 1], (8, T)) for j in range(8)]
        s = [[jnp.broadcast_to(cols[j][i:i + 1, :], (8, T)) if i <= j else None for j in range(8)] for i in range(8)]
        fwd = [p[:, :T], p[:, T:]]
        full = list(fwd)
        pivots = None
        for j in range(8):
            d = s[j][j]
            inv = 1.0 / d
            pivots = d if pivots is None else jnp.where(sub8 == j, d, pivots)
            t = [None if k <= j else s[j][k] * inv for k in range(8)]
            m = [s[i][j] if i <= j else s[j][i] for i in range(8)]
            mcol = m[0]
            for i in range(1, 8):
                mcol = jnp.where(sub8 == i, m[i], mcol)
            for k in range(j + 1, 8):
                for i in range(k + 1):
                    if i != j:
                        s[i][k] = s[i][k] - m[i] * t[k]
                s[j][k] = t[k]
            below = jnp.where(sub8 > j, mcol, 0.0)
            for h in range(2):
                frow = jnp.broadcast_to(fwd[h][j:j + 1, :], (8, T)) * inv
                fwd[h] = fwd[h] - below * frow
                grow = jnp.broadcast_to(full[h][j:j + 1, :], (8, T)) * inv
                full[h] = jnp.where(sub8 == j, grow, full[h] - mcol * grow)
        scale = lax.rsqrt(pivots)
        for h in range(2):
            u_ref[r0:r0 + 8, h * T:(h + 1) * T] = fwd[h] * scale
        if r0 + 8 < T:
            z = jnp.concatenate(full, axis=1)
            parts = []
            if r0:
                parts.append(jnp.zeros((r0, 2 * T), jnp.float32))
            parts.append(z)
            parts.append(jnp.zeros((T - r0 - 8, 2 * T), jnp.float32))
            z = jnp.concatenate(parts, axis=0)
            rest = a_ref[r0 + 8:, :]
            a_ref[r0 + 8:, :] = rest - lax.dot_general(rest[:, :T], z, NN, precision=HIGHEST, preferred_element_type=jnp.float32)

def chol_kernel(g_ref, out_ref, a_ref, u_ref):
    n = g_ref.shape[0]
    steps = n // T
    row = lax.broadcasted_iota(jnp.int32, (T, T), 0)
    col = lax.broadcasted_iota(jnp.int32, (T, T), 1)
    eye = (row == col).astype(jnp.float32)
    for k in range(steps - 1):
        out_ref[k * T:(k + 1) * T, (k + 1) * T:] = jnp.zeros((T, n - (k + 1) * T), jnp.float32)

    def panel(k, carry):
        here = pl.ds(pl.multiple_of(k * T, T), T)
        a_ref[:, :T] = g_ref[here, here]
        a_ref[:, T:] = eye
        factor_block(a_ref, u_ref)
        out_ref[here, here] = jnp.where(row >= col, u_ref[:, :T].T, 0.0)
        for kk in range(steps - 1):
            @pl.when(k == kk)
            def _():
                c = slice(kk * T, (kk + 1) * T)
                lo = (kk + 1) * T
                solved = lax.dot_general(g_ref[lo:, c], u_ref[:, T:], NT, precision=HIGHEST, preferred_element_type=jnp.float32)
                out_ref[lo:, c] = solved
                for j in range(kk + 1, steps):
                    b = slice(j * T, (j + 1) * T)
                    g_ref[j * T:, b] = g_ref[j * T:, b] - lax.dot_general(
                        out_ref[j * T:, c], out_ref[b, c], NT, precision=HIGHEST, preferred_element_type=jnp.float32)
        return carry
    lax.fori_loop(0, steps, panel, 0)

def chol_whole(g_in, o_ref, g_ref, a_ref, u_ref, sem):
    cp = pltpu.make_async_copy(g_in, g_ref, sem)
    cp.start(); cp.wait()
    chol_kernel(g_ref, o_ref, a_ref, u_ref)

def cholesky(g):
    n = g.shape[0]
    return pl.pallas_call(
        chol_whole,
        out_shape=jax.ShapeDtypeStruct((n, n), jnp.float32),
        in_specs=[pl.BlockSpec(memory_space=pl.ANY)],
        out_specs=pl.BlockSpec(memory_space=pltpu.VMEM),
        scratch_shapes=[pltpu.VMEM((n, n), jnp.float32), pltpu.VMEM((T, 2 * T), jnp.float32), pltpu.VMEM((T, 2 * T), jnp.float32), pltpu.SemaphoreType.DMA],
        compiler_params=pltpu.CompilerParams(vmem_limit_bytes=40 * 2**20),
    )(g)


def hadamard_table(extent):
    line_ids = jnp.arange(extent, dtype=jnp.int32)
    correlation = jnp.bitwise_and(line_ids[:, None], line_ids[None, :])
    parity = jnp.zeros((extent, extent), jnp.int32)
    for bit_pos in range(extent.bit_length() - 1):
        parity = parity + jnp.bitwise_and(jnp.right_shift(correlation, bit_pos), 1)
    return (1 - 2 * (parity % 2)).astype(jnp.float32)


def local_transform(values):
    rows_here, columns = values.shape
    inner_size = min(rows_here, 128)
    outer_size = rows_here // inner_size
    blocks = values.reshape(outer_size, inner_size, columns)
    blocks = jnp.einsum("ab,qbn->qan", hadamard_table(inner_size), blocks, precision=HIGHEST)
    blocks = jnp.einsum("pq,qan->pan", hadamard_table(outer_size), blocks, precision=HIGHEST)
    return blocks.reshape(rows_here, columns)


def mix_sources(received):
    return jnp.einsum("ab,bjn->ajn", hadamard_table(received.shape[0]), received, precision=HIGHEST)


def body(matrix, sign_bits, samples):
    rows_here, columns = matrix.shape
    devices = lax.axis_size(("rows", "sub"))
    position = lax.axis_index(("rows", "sub"))
    per_block = rows_here // devices
    sign_values = (2 * sign_bits - 1).astype(jnp.float32)
    current = local_transform(matrix * sign_values[:, None])
    block_ids = (
        (jnp.arange(devices, dtype=jnp.int32) * rows_here)[:, None]
        + position * per_block
        + jnp.arange(per_block, dtype=jnp.int32)[None, :]
    )
    blocks = current.reshape(devices, per_block, columns)
    mixed_rows = mix_sources(
        lax.all_to_all(blocks, ("rows", "sub"), split_axis=0, concat_axis=0, tiled=True)
    )
    owned_rows = mixed_rows.reshape(rows_here, columns)
    row_ids = block_ids.reshape(rows_here)
    matches = (row_ids[:, None] == samples[None, :]).astype(jnp.float32)
    counts = jnp.sum(matches, axis=1)
    weighted = owned_rows * counts[:, None]
    total_rows = rows_here * devices
    own_terms = jnp.einsum("rn,rm->nm", weighted, owned_rows, precision=HIGHEST) / jnp.float32(
        total_rows * samples.shape[0]
    )
    gram_matrix = lax.psum(own_terms, ("rows", "sub"))
    return cholesky(gram_matrix)


def solution(mesh):
    placed = (P(("groups", "rows", "sub"), None), P(("groups", "rows", "sub")), P("groups"))
    return jax.shard_map(
        body, mesh=mesh, in_specs=placed, out_specs=P("groups", None), check_vma=False
    )
```

```python
import functools

import jax
import jax.numpy as jnp
from jax import lax
from jax.experimental import pallas as pl
from jax.experimental.pallas import tpu as pltpu
from jax.sharding import PartitionSpec as P

HIGHEST = lax.Precision.HIGHEST
VMEM = pl.BlockSpec(memory_space=pltpu.VMEM)
T = 128
NT = (((1,), (1,)), ((), ()))
NN = (((1,), (0,)), ((), ()))

def factor_block(a_ref, u_ref):
    sub8 = lax.broadcasted_iota(jnp.int32, (8, T), 0)
    for r0 in range(0, T, 8):
        p = a_ref[r0:r0 + 8, :]
        left = p[:, :T]
        cols = [jnp.broadcast_to(left[:, r0 + j:r0 + j + 1], (8, T)) for j in range(8)]
        s = [[jnp.broadcast_to(cols[j][i:i + 1, :], (8, T)) if i <= j else None for j in range(8)] for i in range(8)]
        fwd = [p[:, :T], p[:, T:]]
        full = list(fwd)
        pivots = None
        for j in range(8):
            d = s[j][j]
            inv = 1.0 / d
            pivots = d if pivots is None else jnp.where(sub8 == j, d, pivots)
            t = [None if k <= j else s[j][k] * inv for k in range(8)]
            m = [s[i][j] if i <= j else s[j][i] for i in range(8)]
            mcol = m[0]
            for i in range(1, 8):
                mcol = jnp.where(sub8 == i, m[i], mcol)
            for k in range(j + 1, 8):
                for i in range(k + 1):
                    if i != j:
                        s[i][k] = s[i][k] - m[i] * t[k]
                s[j][k] = t[k]
            below = jnp.where(sub8 > j, mcol, 0.0)
            for h in range(2):
                frow = jnp.broadcast_to(fwd[h][j:j + 1, :], (8, T)) * inv
                fwd[h] = fwd[h] - below * frow
                grow = jnp.broadcast_to(full[h][j:j + 1, :], (8, T)) * inv
                full[h] = jnp.where(sub8 == j, grow, full[h] - mcol * grow)
        scale = lax.rsqrt(pivots)
        for h in range(2):
            u_ref[r0:r0 + 8, h * T:(h + 1) * T] = fwd[h] * scale
        if r0 + 8 < T:
            z = jnp.concatenate(full, axis=1)
            parts = []
            if r0:
                parts.append(jnp.zeros((r0, 2 * T), jnp.float32))
            parts.append(z)
            parts.append(jnp.zeros((T - r0 - 8, 2 * T), jnp.float32))
            z = jnp.concatenate(parts, axis=0)
            rest = a_ref[r0 + 8:, :]
            a_ref[r0 + 8:, :] = rest - lax.dot_general(rest[:, :T], z, NN, precision=HIGHEST, preferred_element_type=jnp.float32)


def panel_start(j, steps):
    return T * (j * steps - j * (j - 1) // 2)


def chol_kernel(g_in, out_ref, g_ref, a_ref, u_ref, sem):
    n = out_ref.shape[0]
    steps = n // T
    copy = pltpu.make_async_copy(g_in, g_ref, sem)
    copy.start()
    row = lax.broadcasted_iota(jnp.int32, (T, T), 0)
    col = lax.broadcasted_iota(jnp.int32, (T, T), 1)
    eye = (row == col).astype(jnp.float32)
    for k in range(steps - 1):
        out_ref[k * T:(k + 1) * T, (k + 1) * T:] = jnp.zeros((T, n - (k + 1) * T), jnp.float32)
    copy.wait()

    def panel(k, carry):
        here = pl.ds(pl.multiple_of(k * T, T), T)
        a_ref[:, :T] = g_ref[pl.ds(pl.multiple_of(panel_start(k, steps), T), T), :]
        a_ref[:, T:] = eye
        factor_block(a_ref, u_ref)
        out_ref[here, here] = jnp.where(row >= col, u_ref[:, :T].T, 0.0)
        for kk in range(steps - 1):
            @pl.when(k == kk)
            def _():
                c = slice(kk * T, (kk + 1) * T)
                lo = (kk + 1) * T
                start = panel_start(kk, steps)
                out_ref[lo:, c] = lax.dot_general(
                    g_ref[start + T:start + (steps - kk) * T, :], u_ref[:, T:], NT,
                    precision=HIGHEST, preferred_element_type=jnp.float32)
                for j in range(kk + 1, steps):
                    b = slice(panel_start(j, steps), panel_start(j + 1, steps))
                    g_ref[b, :] = g_ref[b, :] - lax.dot_general(
                        out_ref[j * T:, c], out_ref[j * T:(j + 1) * T, c], NT,
                        precision=HIGHEST, preferred_element_type=jnp.float32)
        return carry

    lax.fori_loop(0, steps, panel, 0)


def cholesky(packed, n):
    return pl.pallas_call(
        chol_kernel,
        out_shape=jax.ShapeDtypeStruct((n, n), jnp.float32),
        in_specs=[pl.BlockSpec(memory_space=pl.ANY)],
        out_specs=VMEM,
        scratch_shapes=[
            pltpu.VMEM(packed.shape, jnp.float32),
            pltpu.VMEM((T, 2 * T), jnp.float32),
            pltpu.VMEM((T, 2 * T), jnp.float32),
            pltpu.SemaphoreType.DMA,
        ],
        compiler_params=pltpu.CompilerParams(vmem_limit_bytes=24 * 2**20),
    )(packed)


def butterfly(parts):
    stride = 1
    while stride < len(parts):
        mixed = list(parts)
        for i in range(len(parts)):
            if not i & stride:
                mixed[i] = parts[i] + parts[i + stride]
                mixed[i + stride] = parts[i] - parts[i + stride]
        parts = mixed
        stride *= 2
    return parts


def transform_kernel(x_ref, s_ref, o_ref):
    count, inner = s_ref.shape
    i = lax.broadcasted_iota(jnp.int32, (inner, inner), 0)
    j = lax.broadcasted_iota(jnp.int32, (inner, inner), 1)
    common = i & j
    parity = jnp.zeros((inner, inner), jnp.int32)
    for bit in range(inner.bit_length() - 1):
        parity = parity ^ ((common >> bit) & 1)
    table = (1 - 2 * parity).astype(jnp.float32)
    width = x_ref.shape[1] // 4
    for c in range(4):
        cols = slice(c * width, (c + 1) * width)
        parts = [
            lax.dot_general(table * s_ref[q:q + 1, :], x_ref[q * inner:(q + 1) * inner, cols], NN,
                            precision=HIGHEST, preferred_element_type=jnp.float32)
            for q in range(count)
        ]
        for q, part in enumerate(butterfly(parts)):
            o_ref[q * inner:(q + 1) * inner, cols] = part


def gram_kernel(devices, scale, r_ref, w_ref, o_ref, x_ref, t_ref):
    rows, n = x_ref.shape
    steps = n // T
    height = rows // devices
    piece = 8 if height % 8 == 0 else height
    def mix(step, carry):
        for c in range(steps):
            cols = slice(c * T, (c + 1) * T)
            at = [pl.ds(d * height + step * piece, piece) for d in range(devices)]
            if piece == 8:
                at = [pl.ds(pl.multiple_of(d * height + step * piece, 8), 8) for d in range(devices)]
            for ref_at, part in zip(at, butterfly([r_ref[a, cols] for a in at])):
                x_ref[ref_at, cols] = part
        return carry
    lax.fori_loop(0, height // piece, mix, 0)
    for c in range(steps):
        cols = slice(c * T, (c + 1) * T)
        t_ref[cols, :] = x_ref[:, cols].T * (w_ref[...] * scale)
    for j in range(steps):
        start, stop = panel_start(j, steps), panel_start(j + 1, steps)
        o_ref[start:stop, :] = lax.dot_general(
            t_ref[j * T:, :], x_ref[:, j * T:(j + 1) * T], NN,
            precision=HIGHEST, preferred_element_type=jnp.float32)
    used = panel_start(steps, steps)
    if used < o_ref.shape[0]:
        o_ref[used:, :] = jnp.zeros((o_ref.shape[0] - used, T), jnp.float32)


def gram_panels(received, counts, devices, scale, padded):
    rows, n = received.shape
    if (rows // devices) % 8:
        received = jnp.einsum("ab,bjn->ajn", hadamard_table(devices),
                              received.reshape(devices, rows // devices, n), precision=HIGHEST).reshape(rows, n)
        mixers = 1
    else:
        mixers = devices
    return pl.pallas_call(
        functools.partial(gram_kernel, mixers, scale),
        out_shape=jax.ShapeDtypeStruct((padded, T), jnp.float32),
        in_specs=[VMEM, VMEM],
        out_specs=VMEM,
        scratch_shapes=[pltpu.VMEM((rows, n), jnp.float32), pltpu.VMEM((n, rows), jnp.float32)],
        compiler_params=pltpu.CompilerParams(vmem_limit_bytes=32 * 2**20),
    )(received, counts)


def reduce_kernel(orders, rows_of_part, in_ref, out_ref, sum_ref, got_ref, send_sems, recv_sems):
    rows_id, sub_id, group_id = lax.axis_index("rows"), lax.axis_index("sub"), lax.axis_index("groups")

    def partner(axis, bit):
        mine = rows_id if axis == "rows" else sub_id
        low = lax.rem(mine // bit, 2)
        other = mine + bit * (1 - 2 * low)
        ids = (group_id, other, sub_id) if axis == "rows" else (group_id, rows_id, other)
        return low, ids

    barrier = pltpu.get_barrier_semaphore()
    for axis, bit in orders[0]:
        pl.semaphore_signal(barrier, inc=1, device_id=partner(axis, bit)[1], device_id_type=pl.DeviceIdType.MESH)
    pl.semaphore_wait(barrier, len(orders[0]))

    levels = len(orders[0])
    offsets = [[p * rows_of_part] for p in range(len(orders))]
    size = rows_of_part
    got_at = 0
    for level in range(levels):
        half = size // 2
        sent = []
        for p, order in enumerate(orders):
            low, ids = partner(*order[level])
            base = offsets[p][-1]
            keep = pl.multiple_of(base + low * half, 8)
            give = pl.multiple_of(base + (1 - low) * half, 8)
            slot = got_at + p * half
            source = in_ref if level == 0 else sum_ref
            copy = pltpu.make_async_remote_copy(
                src_ref=source.at[pl.ds(give, half)], dst_ref=got_ref.at[slot:slot + half],
                send_sem=send_sems.at[level, p], recv_sem=recv_sems.at[level, p],
                device_id=ids, device_id_type=pl.DeviceIdType.MESH)
            copy.start()
            sent.append((copy, keep, slot))
            offsets[p].append(keep)
        for copy, keep, slot in sent:
            copy.wait()
            source = in_ref if level == 0 else sum_ref
            target = out_ref if level == levels - 1 else sum_ref
            target[pl.ds(keep, half), :] = source[pl.ds(keep, half), :] + got_ref[slot:slot + half, :]
        got_at += half * len(orders)
        size = half
    for level in range(levels - 1, -1, -1):
        sent = []
        for p, order in enumerate(orders):
            low, ids = partner(*order[level])
            region = pl.ds(offsets[p][level + 1], size)
            copy = pltpu.make_async_remote_copy(
                src_ref=out_ref.at[region], dst_ref=out_ref.at[region],
                send_sem=send_sems.at[levels + level, p], recv_sem=recv_sems.at[levels + level, p],
                device_id=ids, device_id_type=pl.DeviceIdType.MESH)
            copy.start()
            sent.append(copy)
        for copy in sent:
            copy.wait()
        size *= 2


def all_reduce(panels, mesh_sizes):
    sub_bits = [("sub", 1 << b) for b in range(mesh_sizes["sub"].bit_length() - 1)]
    row_bits = [("rows", 1 << b) for b in range(mesh_sizes["rows"].bit_length() - 1)]
    orders = (tuple(sub_bits + row_bits), tuple(sub_bits[:1] + row_bits + sub_bits[1:]))
    levels = len(orders[0])
    rows = panels.shape[0]
    return pl.pallas_call(
        functools.partial(reduce_kernel, orders, rows // 2),
        out_shape=jax.ShapeDtypeStruct(panels.shape, jnp.float32),
        in_specs=[VMEM],
        out_specs=VMEM,
        scratch_shapes=[
            pltpu.VMEM(panels.shape, jnp.float32),
            pltpu.VMEM(panels.shape, jnp.float32),
            pltpu.SemaphoreType.DMA((2 * levels, 2)),
            pltpu.SemaphoreType.DMA((2 * levels, 2)),
        ],
        compiler_params=pltpu.CompilerParams(
            collective_id=0, has_side_effects=True, vmem_limit_bytes=24 * 2**20),
    )(panels)


def hadamard_table(extent):
    line_ids = jnp.arange(extent, dtype=jnp.int32)
    correlation = jnp.bitwise_and(line_ids[:, None], line_ids[None, :])
    parity = jnp.zeros((extent, extent), jnp.int32)
    for bit_pos in range(extent.bit_length() - 1):
        parity = parity + jnp.bitwise_and(jnp.right_shift(correlation, bit_pos), 1)
    return (1 - 2 * (parity % 2)).astype(jnp.float32)


def body(mesh_sizes, matrix, sign_bits, samples):
    rows_here, columns = matrix.shape
    devices = mesh_sizes["rows"] * mesh_sizes["sub"]
    position = lax.axis_index(("rows", "sub"))
    per_block = rows_here // devices
    inner = min(rows_here, 128)
    signs = (2 * sign_bits - 1).astype(jnp.float32).reshape(rows_here // inner, inner)
    current = pl.pallas_call(
        transform_kernel,
        out_shape=jax.ShapeDtypeStruct(matrix.shape, jnp.float32),
        in_specs=[VMEM, VMEM],
        out_specs=VMEM,
        compiler_params=pltpu.CompilerParams(vmem_limit_bytes=24 * 2**20),
    )(matrix, signs)
    blocks = current.reshape(devices, per_block, columns)
    received = lax.all_to_all(blocks, ("rows", "sub"), split_axis=0, concat_axis=0, tiled=True)
    line = jnp.arange(rows_here, dtype=jnp.int32)
    row_ids = (line // per_block) * rows_here + position * per_block + line % per_block
    counts = jnp.sum((row_ids[:, None] == samples[None, :]).astype(jnp.float32), axis=1)
    total_rows = rows_here * devices
    scale = 1.0 / (total_rows * samples.shape[0])
    steps = columns // T
    unit = 16 * devices
    padded = -(-panel_start(steps, steps) // unit) * unit
    panels = gram_panels(received.reshape(rows_here, columns), counts[None, :], devices, scale, padded)
    return cholesky(all_reduce(panels, mesh_sizes), columns)


def solution(mesh):
    placed = (P(("groups", "rows", "sub"), None), P(("groups", "rows", "sub")), P("groups"))
    return jax.shard_map(
        functools.partial(body, dict(mesh.shape)), mesh=mesh, in_specs=placed, out_specs=P("groups", None),
        check_vma=False
    )
```

```python
import functools

import jax
import jax.numpy as jnp
from jax import lax
from jax.experimental import pallas as pl
from jax.experimental.pallas import tpu as pltpu
from jax.sharding import PartitionSpec as P

HIGHEST = lax.Precision.HIGHEST
VMEM = pl.BlockSpec(memory_space=pltpu.VMEM)
T = 128
NT = (((1,), (1,)), ((), ()))
NN = (((1,), (0,)), ((), ()))

def factor_block(a_ref, u_ref):
    sub8 = lax.broadcasted_iota(jnp.int32, (8, T), 0)
    p = [a_ref[0:8, :T], a_ref[0:8, T:]]
    for r0 in range(0, T, 8):
        left = p[0]
        if r0 + 8 < T:
            after = [a_ref[r0 + 8:r0 + 16, :T], a_ref[r0 + 8:r0 + 16, T:]]
            after_cols = [jnp.broadcast_to(after[0][:, r0 + j:r0 + j + 1], (8, T)) for j in range(8)]
        cols = [jnp.broadcast_to(left[:, r0 + j:r0 + j + 1], (8, T)) for j in range(8)]
        s = [[jnp.broadcast_to(cols[j][i:i + 1, :], (8, T)) if i <= j else None for j in range(8)] for i in range(8)]
        fwd = list(p)
        full = list(fwd)
        pivots = None
        for j in range(8):
            d = s[j][j]
            inv = 1.0 / d
            pivots = d if pivots is None else jnp.where(sub8 == j, d, pivots)
            t = [None if k <= j else s[j][k] * inv for k in range(8)]
            m = [s[i][j] if i <= j else s[j][i] for i in range(8)]
            mcol = m[0]
            for i in range(1, 8):
                mcol = jnp.where(sub8 == i, m[i], mcol)
            for k in range(j + 1, 8):
                for i in range(k + 1):
                    if i != j:
                        s[i][k] = s[i][k] - m[i] * t[k]
                s[j][k] = t[k]
            for h in range(2):
                fwd[h] = jnp.where(sub8 == j, full[h], fwd[h])
                grow = jnp.broadcast_to(full[h][j:j + 1, :], (8, T)) * inv
                full[h] = jnp.where(sub8 == j, grow, full[h] - mcol * grow)
        scale = lax.rsqrt(pivots)
        for h in range(2):
            u_ref[r0:r0 + 8, h * T:(h + 1) * T] = fwd[h] * scale
        if r0 + 8 < T:
            for j in range(8):
                for h in range(2):
                    after[h] = after[h] - after_cols[j] * jnp.broadcast_to(full[h][j:j + 1, :], (8, T))
            p = after
        if r0 + 16 < T:
            z = jnp.concatenate(full, axis=1)
            parts = []
            if r0:
                parts.append(jnp.zeros((r0, 2 * T), jnp.float32))
            parts.append(z)
            parts.append(jnp.zeros((T - r0 - 8, 2 * T), jnp.float32))
            z = jnp.concatenate(parts, axis=0)
            rest = a_ref[r0 + 16:, :]
            a_ref[r0 + 16:, :] = rest - lax.dot_general(rest[:, :T], z, NN, precision=HIGHEST, preferred_element_type=jnp.float32)


def panel_start(j, steps):
    return T * (j * steps - j * (j - 1) // 2)


def chol_kernel(g_in, out_ref, g_ref, a_ref, u_ref, sem):
    n = out_ref.shape[0]
    steps = n // T
    copy = pltpu.make_async_copy(g_in, g_ref, sem)
    copy.start()
    row = lax.broadcasted_iota(jnp.int32, (T, T), 0)
    col = lax.broadcasted_iota(jnp.int32, (T, T), 1)
    eye = (row == col).astype(jnp.float32)
    for k in range(steps - 1):
        out_ref[k * T:(k + 1) * T, (k + 1) * T:] = jnp.zeros((T, n - (k + 1) * T), jnp.float32)
    copy.wait()

    def panel(k, carry):
        here = pl.ds(pl.multiple_of(k * T, T), T)
        a_ref[:, :T] = g_ref[pl.ds(pl.multiple_of(panel_start(k, steps), T), T), :]
        a_ref[:, T:] = eye
        factor_block(a_ref, u_ref)
        out_ref[here, here] = jnp.where(row >= col, u_ref[:, :T].T, 0.0)
        for kk in range(steps - 1):
            @pl.when(k == kk)
            def _():
                c = slice(kk * T, (kk + 1) * T)
                lo = (kk + 1) * T
                start = panel_start(kk, steps)
                out_ref[lo:, c] = lax.dot_general(
                    g_ref[start + T:start + (steps - kk) * T, :], u_ref[:, T:], NT,
                    precision=HIGHEST, preferred_element_type=jnp.float32)
                for j in range(kk + 1, steps):
                    b = slice(panel_start(j, steps), panel_start(j + 1, steps))
                    g_ref[b, :] = g_ref[b, :] - lax.dot_general(
                        out_ref[j * T:, c], out_ref[j * T:(j + 1) * T, c], NT,
                        precision=HIGHEST, preferred_element_type=jnp.float32)
        return carry

    lax.fori_loop(0, steps, panel, 0)


def cholesky(packed, n):
    return pl.pallas_call(
        chol_kernel,
        out_shape=jax.ShapeDtypeStruct((n, n), jnp.float32),
        in_specs=[pl.BlockSpec(memory_space=pl.ANY)],
        out_specs=VMEM,
        scratch_shapes=[
            pltpu.VMEM(packed.shape, jnp.float32),
            pltpu.VMEM((T, 2 * T), jnp.float32),
            pltpu.VMEM((T, 2 * T), jnp.float32),
            pltpu.SemaphoreType.DMA,
        ],
        compiler_params=pltpu.CompilerParams(vmem_limit_bytes=24 * 2**20),
    )(packed)


def butterfly(parts):
    stride = 1
    while stride < len(parts):
        mixed = list(parts)
        for i in range(len(parts)):
            if not i & stride:
                mixed[i] = parts[i] + parts[i + stride]
                mixed[i + stride] = parts[i] - parts[i + stride]
        parts = mixed
        stride *= 2
    return parts


def transform_kernel(x_ref, s_ref, o_ref):
    count, inner = s_ref.shape
    i = lax.broadcasted_iota(jnp.int32, (inner, inner), 0)
    j = lax.broadcasted_iota(jnp.int32, (inner, inner), 1)
    common = i & j
    parity = jnp.zeros((inner, inner), jnp.int32)
    for bit in range(inner.bit_length() - 1):
        parity = parity ^ ((common >> bit) & 1)
    table = (1 - 2 * parity).astype(jnp.float32)
    width = x_ref.shape[1] // 4
    for c in range(4):
        cols = slice(c * width, (c + 1) * width)
        parts = [
            lax.dot_general(table * s_ref[q:q + 1, :], x_ref[q * inner:(q + 1) * inner, cols], NN,
                            precision=HIGHEST, preferred_element_type=jnp.float32)
            for q in range(count)
        ]
        for q, part in enumerate(butterfly(parts)):
            o_ref[q * inner:(q + 1) * inner, cols] = part


def gram_kernel(devices, scale, r_ref, w_ref, o_ref, x_ref, t_ref):
    rows, n = x_ref.shape
    steps = n // T
    height = rows // devices
    piece = 8 if height % 8 == 0 else height
    def mix(step, carry):
        for c in range(steps):
            cols = slice(c * T, (c + 1) * T)
            at = [pl.ds(d * height + step * piece, piece) for d in range(devices)]
            if piece == 8:
                at = [pl.ds(pl.multiple_of(d * height + step * piece, 8), 8) for d in range(devices)]
            for ref_at, part in zip(at, butterfly([r_ref[a, cols] for a in at])):
                x_ref[ref_at, cols] = part
        return carry
    lax.fori_loop(0, height // piece, mix, 0)
    for c in range(steps):
        cols = slice(c * T, (c + 1) * T)
        t_ref[cols, :] = x_ref[:, cols].T * (w_ref[...] * scale)
    for j in range(steps):
        start, stop = panel_start(j, steps), panel_start(j + 1, steps)
        o_ref[start:stop, :] = lax.dot_general(
            t_ref[j * T:, :], x_ref[:, j * T:(j + 1) * T], NN,
            precision=HIGHEST, preferred_element_type=jnp.float32)
    used = panel_start(steps, steps)
    if used < o_ref.shape[0]:
        o_ref[used:, :] = jnp.zeros((o_ref.shape[0] - used, T), jnp.float32)


def gram_panels(received, counts, devices, scale, padded):
    rows, n = received.shape
    if (rows // devices) % 8:
        received = jnp.einsum("ab,bjn->ajn", hadamard_table(devices),
                              received.reshape(devices, rows // devices, n), precision=HIGHEST).reshape(rows, n)
        mixers = 1
    else:
        mixers = devices
    return pl.pallas_call(
        functools.partial(gram_kernel, mixers, scale),
        out_shape=jax.ShapeDtypeStruct((padded, T), jnp.float32),
        in_specs=[VMEM, VMEM],
        out_specs=VMEM,
        scratch_shapes=[pltpu.VMEM((rows, n), jnp.float32), pltpu.VMEM((n, rows), jnp.float32)],
        compiler_params=pltpu.CompilerParams(vmem_limit_bytes=32 * 2**20),
    )(received, counts)


def reduce_kernel(orders, rows_of_part, in_ref, out_ref, sum_ref, got_ref, send_sems, recv_sems):
    rows_id, sub_id, group_id = lax.axis_index("rows"), lax.axis_index("sub"), lax.axis_index("groups")

    def partner(axis, bit):
        mine = rows_id if axis == "rows" else sub_id
        low = lax.rem(mine // bit, 2)
        other = mine + bit * (1 - 2 * low)
        ids = (group_id, other, sub_id) if axis == "rows" else (group_id, rows_id, other)
        return low, ids

    barrier = pltpu.get_barrier_semaphore()
    for axis, bit in orders[0]:
        pl.semaphore_signal(barrier, inc=1, device_id=partner(axis, bit)[1], device_id_type=pl.DeviceIdType.MESH)
    pl.semaphore_wait(barrier, len(orders[0]))

    levels = len(orders[0])
    offsets = [[p * rows_of_part] for p in range(len(orders))]

    def slot(level, p):
        half = rows_of_part >> (level + 1)
        at = (rows_of_part - (rows_of_part >> level)) * len(orders) + p * half
        return slice(at, at + half)

    def halving(level, p):
        low, ids = partner(*orders[p][level])
        half = rows_of_part >> (level + 1)
        base = offsets[p][level]
        keep = pl.multiple_of(base + low * half, 8)
        give = pl.multiple_of(base + (1 - low) * half, 8)
        offsets[p].append(keep)
        source = in_ref if level == 0 else sum_ref
        copy = pltpu.make_async_remote_copy(
            src_ref=source.at[pl.ds(give, half)], dst_ref=got_ref.at[slot(level, p)],
            send_sem=send_sems.at[level, p], recv_sem=recv_sems.at[level, p],
            device_id=ids, device_id_type=pl.DeviceIdType.MESH)
        copy.start()
        return copy

    def doubling(level, p):
        ids = partner(*orders[p][level])[1]
        region = pl.ds(offsets[p][level + 1], rows_of_part >> (level + 1))
        copy = pltpu.make_async_remote_copy(
            src_ref=out_ref.at[region], dst_ref=out_ref.at[region],
            send_sem=send_sems.at[levels + level, p], recv_sem=recv_sems.at[levels + level, p],
            device_id=ids, device_id_type=pl.DeviceIdType.MESH)
        copy.start()
        return copy

    parts = range(len(orders))
    flying = [halving(0, p) for p in parts]
    for level in range(levels):
        for p in parts:
            flying[p].wait()
            source = in_ref if level == 0 else sum_ref
            target = out_ref if level == levels - 1 else sum_ref
            kept = pl.ds(offsets[p][level + 1], rows_of_part >> (level + 1))
            target[kept, :] = source[kept, :] + got_ref[slot(level, p), :]
            flying[p] = halving(level + 1, p) if level < levels - 1 else doubling(level, p)
    for level in range(levels - 1, -1, -1):
        for p in parts:
            flying[p].wait()
            if level:
                flying[p] = doubling(level - 1, p)


def all_reduce(panels, mesh_sizes):
    sub_bits = [("sub", 1 << b) for b in range(mesh_sizes["sub"].bit_length() - 1)]
    row_bits = [("rows", 1 << b) for b in range(mesh_sizes["rows"].bit_length() - 1)]
    orders = (tuple(sub_bits + row_bits), tuple(sub_bits[:1] + row_bits + sub_bits[1:]))
    orders = orders + orders
    levels = len(orders[0])
    rows = panels.shape[0]
    return pl.pallas_call(
        functools.partial(reduce_kernel, orders, rows // len(orders)),
        out_shape=jax.ShapeDtypeStruct(panels.shape, jnp.float32),
        in_specs=[VMEM],
        out_specs=VMEM,
        scratch_shapes=[
            pltpu.VMEM(panels.shape, jnp.float32),
            pltpu.VMEM(panels.shape, jnp.float32),
            pltpu.SemaphoreType.DMA((2 * levels, len(orders))),
            pltpu.SemaphoreType.DMA((2 * levels, len(orders))),
        ],
        compiler_params=pltpu.CompilerParams(
            collective_id=0, has_side_effects=True, vmem_limit_bytes=24 * 2**20),
    )(panels)


def hadamard_table(extent):
    line_ids = jnp.arange(extent, dtype=jnp.int32)
    correlation = jnp.bitwise_and(line_ids[:, None], line_ids[None, :])
    parity = jnp.zeros((extent, extent), jnp.int32)
    for bit_pos in range(extent.bit_length() - 1):
        parity = parity + jnp.bitwise_and(jnp.right_shift(correlation, bit_pos), 1)
    return (1 - 2 * (parity % 2)).astype(jnp.float32)


def body(mesh_sizes, matrix, sign_bits, samples):
    rows_here, columns = matrix.shape
    devices = mesh_sizes["rows"] * mesh_sizes["sub"]
    position = lax.axis_index(("rows", "sub"))
    per_block = rows_here // devices
    inner = min(rows_here, 128)
    signs = (2 * sign_bits - 1).astype(jnp.float32).reshape(rows_here // inner, inner)
    current = pl.pallas_call(
        transform_kernel,
        out_shape=jax.ShapeDtypeStruct(matrix.shape, jnp.float32),
        in_specs=[VMEM, VMEM],
        out_specs=VMEM,
        compiler_params=pltpu.CompilerParams(vmem_limit_bytes=24 * 2**20),
    )(matrix, signs)
    blocks = current.reshape(devices, per_block, columns)
    received = lax.all_to_all(blocks, ("rows", "sub"), split_axis=0, concat_axis=0, tiled=True)
    line = jnp.arange(rows_here, dtype=jnp.int32)
    row_ids = (line // per_block) * rows_here + position * per_block + line % per_block
    counts = jnp.sum((row_ids[:, None] == samples[None, :]).astype(jnp.float32), axis=1)
    total_rows = rows_here * devices
    scale = 1.0 / (total_rows * samples.shape[0])
    steps = columns // T
    unit = 32 * devices
    padded = -(-panel_start(steps, steps) // unit) * unit
    panels = gram_panels(received.reshape(rows_here, columns), counts[None, :], devices, scale, padded)
    return cholesky(all_reduce(panels, mesh_sizes), columns)


def solution(mesh):
    placed = (P(("groups", "rows", "sub"), None), P(("groups", "rows", "sub")), P("groups"))
    return jax.shard_map(
        functools.partial(body, dict(mesh.shape)), mesh=mesh, in_specs=placed, out_specs=P("groups", None),
        check_vma=False
    )
```
